32 devices in a mesh: grp: 2 (over x), lon: 4 (over y, core), lat: 4 (over z).
Axes of the slice: x: 2, y: 2, z: 4, core: 2. Of those that a mesh axis runs over, the one named last changes fastest.
Arguments:
- fields: bfloat16 [6, 2, 48, 48, 512], P('grp', None, 'lat', 'lon'), may hold values from -6 to 6
- surface_mask: int32 [2, 48, 48], P(None, 'lat', 'lon'), may hold values 0 or 1
- w_qkv: bfloat16 [512, 1536], replicated, may hold values from -0.25 to 0.25
- w_out: bfloat16 [512, 512], replicated, may hold values from -0.25 to 0.25
- logit_scale: float32 [8], replicated, may hold values from 2 to 12
- mask_bias: float32 [8], replicated, may hold values from -2 to 2
- w_up: bfloat16 [512, 2048], replicated, may hold values from -0.25 to 0.25
- w_down: bfloat16 [2048, 512], replicated, may hold values from -0.125 to 0.125
Outputs:
- joined: bfloat16 [6, 2, 48, 48, 512], P('grp', None, 'lat', 'lon')
The draws below stay inside these ranges and needn't reach their ends.
All inputs are finite; a program needn't handle non-finite values. No bound on the sum of `surface_mask` on one device may be relied on, other than what follows from the above.
Results may differ from the reference program's by a relative error of at most 0.006.
Values may be sent and summed in bfloat16 or wider, within the bound.
A program may use at most 128 MiB of HBM per device.

```python
import math
import jax
import jax.numpy as jnp
from jax import lax

G = 6
LEV = 2
C = 512
HEADS = 8
HIDDEN_SIZE = 2048
WLAT = 6
WLON = 12
SH_LAT = 3
SH_LON = 6
NLAT = 48
NLON = 48


def plant(array, rng, least, largest):
    index_at = [jax.random.randint(jax.random.fold_in(rng, axis), (), 0, length) for axis, length in enumerate(array.shape)]
    main_axis = array.shape.index(max(array.shape))
    neighbour = index_at[:main_axis] + [(index_at[main_axis] + 1) % array.shape[main_axis]] + index_at[main_axis + 1:]
    return array.at[tuple(index_at)].set(least).at[tuple(neighbour)].set(largest)


def level_of(key, extent, pieces, least, largest):
    loudness = 1.0
    for position, shards_of in pieces:
        heights = jax.random.uniform(jax.random.fold_in(jax.random.fold_in(key, 6), position), (shards_of,), jnp.float32, least / len(pieces), largest / len(pieces))
        loudness = loudness * jnp.repeat(jnp.exp(heights), extent[position] // shards_of).reshape((-1,) + (1,) * (len(extent) - 1 - position))
    return loudness


def bell_draw(key, shape, deviation, limit, split=(), kind=jnp.bfloat16):
    array = jax.random.normal(key, shape, jnp.float32) * deviation
    if len(split) > 0:
        array = level_of(key, shape, split, -0.22, 0.18) * array
    return jnp.clip(array, min=-limit, max=limit).astype(kind)


def setup_inputs(seed: int = 0) -> dict:
    seeds = jax.random.split(jax.random.key(seed), 9)
    fields = bell_draw(seeds[0], (G, LEV, NLAT, NLON, C), 1.0, 6.0, ((0, 2), (2, 4), (3, 4)))
    surface_mask = plant((jax.random.randint(seeds[1], (LEV, NLAT, NLON), 0, 2) < 1).astype(jnp.int32), jax.random.fold_in(seeds[1], 1), 0, 1)
    w_qkv = bell_draw(seeds[2], (C, 3 * C), C ** -0.5, 0.25)
    w_out = bell_draw(seeds[3], (C, C), C ** -0.5, 0.25)
    logit_scale = jnp.clip(jnp.exp(jax.random.uniform(seeds[4], (HEADS,), jnp.float32, math.log(2.0), math.log(12.0))), 2.0, 12.0)
    mask_bias = jnp.clip(jax.random.uniform(seeds[5], (HEADS,), jnp.float32, -2.0, 2.0), -2.0, 2.0)
    w_up = bell_draw(seeds[6], (C, HIDDEN_SIZE), C ** -0.5, 0.25)
    w_down = bell_draw(seeds[7], (HIDDEN_SIZE, C), HIDDEN_SIZE ** -0.5, 0.125)
    return {"fields": fields, "surface_mask": surface_mask, "w_qkv": w_qkv, "w_out": w_out, "logit_scale": logit_scale, "mask_bias": mask_bias, "w_up": w_up, "w_down": w_down}


def layer_norm(values):
    centred = values - lax.optimization_barrier(jnp.mean(values, -1, keepdims=True))
    return centred * lax.rsqrt(lax.optimization_barrier(jnp.mean(centred * centred, -1, keepdims=True)) + 1e-05)

def unit_heads(mixed_part, head_count):
    shaped = mixed_part.reshape(mixed_part.shape[0], head_count, -1)
    scaled = shaped * lax.rsqrt(lax.optimization_barrier(jnp.mean(shaped * shaped, -1, keepdims=True)) + 1e-06)
    return scaled.reshape(mixed_part.shape).astype(jnp.bfloat16)

def windowed(tensor, nlat, nlon):
    lead = tensor.shape[:2]
    rest = tensor.shape[4:]
    shaped = tensor.reshape(lead + (nlat // WLAT, WLAT, nlon // WLON, WLON) + rest)
    order = (2, 4, 0, 1, 3, 5) + tuple(range(6, 6 + len(rest)))
    moved = jnp.transpose(shaped, order)
    return moved.reshape((nlat // WLAT * (nlon // WLON), lead[0] * lead[1] * WLAT * WLON) + rest)

def attend_window(window_args, scale, head_count):
    query_win, key_win, value_win, bias_win, region_win = window_args
    tokens, model_width = query_win.shape
    head_size = model_width // head_count
    query_heads = query_win.astype(jnp.float32).reshape(tokens, head_count, head_size)
    key_heads = key_win.astype(jnp.float32).reshape(tokens, head_count, head_size)
    value_heads = value_win.astype(jnp.float32).reshape(tokens, head_count, head_size)
    scores = jnp.einsum('qhd,khd->hqk', query_heads, key_heads)
    scores = scores * (scale / head_size)[:, None, None] + bias_win[:, None, :]
    same_region = region_win[:, None] == region_win[None, :]
    weights = jnp.where(same_region[None], jnp.exp(scores), 0.0).astype(jnp.bfloat16)
    weights = lax.optimization_barrier(weights).astype(jnp.float32)
    totals = lax.optimization_barrier(jnp.sum(weights, -1))
    weighted = jnp.einsum('hqk,khd->qhd', weights, value_heads)
    ratio = weighted / jnp.transpose(totals)[:, :, None]
    return ratio.astype(jnp.bfloat16).reshape(tokens, model_width)

def reference(fields, surface_mask, w_qkv, w_out, logit_scale, mask_bias, w_up, w_down):
    groups, levels, nlat, nlon, model_width = fields.shape
    head_count = logit_scale.shape[0]
    rolled = jnp.roll(fields, (-SH_LAT, -SH_LON), axis=(2, 3))
    marks = jnp.roll(surface_mask, (-SH_LAT, -SH_LON), axis=(1, 2)).astype(jnp.float32)
    normed = layer_norm(rolled.astype(jnp.float32)).astype(jnp.bfloat16)
    mixed = jnp.dot(normed.reshape(-1, model_width), w_qkv, preferred_element_type=jnp.float32)
    grid_shape = (groups, levels, nlat, nlon, model_width)
    queries = unit_heads(mixed[:, :model_width], head_count).reshape(grid_shape)
    key_part = unit_heads(mixed[:, model_width:2 * model_width], head_count).reshape(grid_shape)
    value_part = mixed[:, 2 * model_width:].astype(jnp.bfloat16).reshape(grid_shape)
    window_count = nlat // WLAT * (nlon // WLON)
    key_bias = mask_bias[:, None, None, None] * marks[None]
    key_bias = key_bias.reshape(head_count, levels, nlat // WLAT, WLAT, nlon // WLON, WLON)
    key_bias = jnp.transpose(key_bias, (2, 4, 0, 1, 3, 5)).reshape(window_count, head_count, -1)
    key_bias = jnp.tile(key_bias, (1, 1, groups))
    row_ids = jnp.arange(nlat, dtype=jnp.int32)
    flag_rows = (row_ids >= nlat - SH_LAT).astype(jnp.int32)
    flag_grid = jnp.broadcast_to(flag_rows[None, None, :, None], (1, levels, nlat, nlon))
    region_win = jnp.tile(windowed(flag_grid, nlat, nlon), (1, groups))

    def attend_block(window_args):
        return attend_window(window_args, logit_scale, head_count)
    attended = lax.map(attend_block, (windowed(queries, nlat, nlon), windowed(key_part, nlat, nlon), windowed(value_part, nlat, nlon), key_bias, region_win))
    attended = attended.reshape(nlat // WLAT, nlon // WLON, groups, levels, WLAT, WLON, model_width)
    attended = jnp.transpose(attended, (2, 3, 0, 4, 1, 5, 6)).reshape(grid_shape)
    projected = jnp.dot(attended.reshape(-1, model_width), w_out, preferred_element_type=jnp.float32)
    projected = projected.astype(jnp.bfloat16).reshape(grid_shape)
    unrolled = jnp.roll(projected, (SH_LAT, SH_LON), axis=(2, 3))
    residual = (fields.astype(jnp.float32) + unrolled.astype(jnp.float32)).astype(jnp.bfloat16)
    mlp_in = layer_norm(residual.astype(jnp.float32)).astype(jnp.bfloat16)
    hidden = jax.nn.gelu(jnp.dot(mlp_in.reshape(-1, model_width), w_up, preferred_element_type=jnp.float32), approximate=True).astype(jnp.bfloat16)
    update = jnp.dot(hidden, w_down, preferred_element_type=jnp.float32).reshape(grid_shape)
    return (residual.astype(jnp.float32) + update).astype(jnp.bfloat16)
```

```python
import functools
import math

import jax
import jax.numpy as jnp
from jax import lax
from jax.experimental import pallas as pl
from jax.experimental.pallas import tpu as pltpu
from jax.sharding import PartitionSpec as P

SH_LAT = 3
SH_LON = 6
LOG2E = math.log2(math.e)
FAR = -30000.0
MESH = pl.DeviceIdType.MESH
BF16 = jnp.bfloat16
F32 = jnp.float32


def layer_norm(values):
    centred = values - jnp.mean(values, -1, keepdims=True)
    return centred * lax.rsqrt(jnp.mean(centred * centred, -1, keepdims=True) + 1e-05)


def iota(shape, axis):
    return lax.broadcasted_iota(jnp.int32, shape, axis)


def dot(left, right):
    return jnp.dot(left, right, preferred_element_type=F32)


def dot_t(left, right):
    return lax.dot_general(left, right, (((1,), (1,)), ((), ())), preferred_element_type=F32)


def kernel(
    real, heads,
    fields_hbm, mask_hbm, scale_hbm, bias_hbm, wqkv_hbm, wout_hbm, wup_hbm, wdown_hbm,
    out_ref,
    raw, mask_ref, scale_ref, bias_ref, tidy, marked, rin, win, wqkv, wout, wup, wdown, att, qs, ks, vs,
    kx, acc, rout, sort0, sort1, put0, put1, blocks, soft,
    wsem, ssem, msend, mrecv, send1, recv1, send2, recv2,
):
    rows, width = win.shape[2:]
    levels = mask_ref.shape[1]
    nlat = mask_ref.shape[0]
    tiles = width // 128
    side_pairs = SH_LON // 2
    slab = rin.shape[1:]
    slab_rows = slab[0] * slab[1] * slab[2] * slab[3]
    pair_rows = 2 * rows
    half = 2 * pair_rows
    total = 2 * half
    pairs = heads // 2
    head_size = width // heads
    lanes = 2 * head_size
    cut_rows = 256
    cut = cut_rows // tiles

    g, a, b = lax.axis_index("grp"), lax.axis_index("lat"), lax.axis_index("lon")
    na, nb = lax.axis_size("lat"), lax.axis_size("lon")
    mine = (g + b) % 2

    def peer(d, da, db):
        return {"grp": (g + d) % 2, "lat": (a + da + na) % na, "lon": (b + db + nb) % nb}

    barrier = pltpu.get_barrier_semaphore()
    greeted = 0
    for d in (0, 1):
        for da, db in ((0, 0), (-1, 0), (0, -1), (-1, -1), (1, 0), (0, 1), (1, 1)):
            if d or da or db:
                pl.semaphore_signal(barrier, inc=1, device_id=peer(d, da, db), device_id_type=MESH)
                greeted += 1

    def row_of(parity, rr):
        return (1 + 2 * parity + rr) % 4

    def block_of(ref, parity, cc, rr):
        r = row_of(parity, rr)
        return ref.at[:, pl.ds(SH_LAT * r, SH_LAT), pl.ds(side_pairs * (1 - cc), side_pairs)]

    def by_owner(d, cc, rr, local, remote):
        if d or cc:
            remote()
        elif rr == 0:
            if local is not None:
                local()
        else:
            pl.when(mine == 1)(remote)
            if local is not None:
                pl.when(mine == 0)(local)

    def stay(cc, rr):
        i = 2 * rr + cc
        return pltpu.make_async_copy(block_of(fields_hbm, mine, cc, rr), rin.at[i], recv1.at[i])

    def forward(d, cc, rr):
        i = 4 * d + 2 * rr + cc
        parity = (g + b + d + cc) % 2
        return pltpu.make_async_remote_copy(
            src_ref=block_of(raw, parity, cc, rr), dst_ref=rin.at[i],
            send_sem=send1.at[i], recv_sem=recv1.at[i],
            device_id=peer(d, -rr * parity, -cc), device_id_type=MESH,
        )

    def backward(d, cc, rr):
        i = 4 * d + 2 * rr + cc
        return pltpu.make_async_remote_copy(
            src_ref=rout.at[i], dst_ref=block_of(out_ref, mine, cc, rr),
            send_sem=send2.at[i], recv_sem=recv2.at[i],
            device_id=peer(d, rr * mine, cc), device_id_type=MESH,
        )

    def settle(cc, rr):
        i = 2 * rr + cc
        return pltpu.make_async_copy(rout.at[i], block_of(out_ref, mine, cc, rr), recv2.at[i])

    def share(n):
        da, db = ((0, -1), (-1, 0), (-1, -1))[n]
        return pltpu.make_async_remote_copy(
            src_ref=tidy, dst_ref=marked.at[n], send_sem=msend.at[n], recv_sem=mrecv.at[n],
            device_id=peer(0, da, db), device_id_type=MESH,
        )

    load = pltpu.make_async_copy(fields_hbm, raw, wsem.at[4])
    load.start()
    small = [
        pltpu.make_async_copy(src, dst, ssem.at[i])
        for i, (src, dst) in enumerate(
            ((mask_hbm, mask_ref), (scale_hbm, scale_ref), (bias_hbm, bias_ref))
        )
    ]
    for copy in small:
        copy.start()
    stay(0, 0).start()
    pl.when(mine == 0)(lambda: stay(0, 1).start())
    weights = [
        pltpu.make_async_copy(src, dst, wsem.at[i])
        for i, (src, dst) in enumerate(
            ((wqkv_hbm, wqkv), (wout_hbm, wout), (wup_hbm, wup), (wdown_hbm, wdown))
        )
    ]
    for copy in weights:
        copy.start()

    for copy in small:
        copy.wait()
    tidy[...] = jnp.zeros_like(tidy)
    for i in range(nlat):
        tidy[levels * i : levels * (i + 1), : mask_ref.shape[2]] = mask_ref[i].astype(F32)

    load.wait()
    pl.semaphore_wait(barrier, greeted)
    order = [(d, cc, rr) for rr in (0, 1) for cc in (0, 1) for d in (1, 0)]
    for d, cc, rr in order:
        by_owner(d, cc, rr, None, lambda: forward(d, cc, rr).start())
    for n in range(3):
        share(n).start()

    def shuffle(count, held, out_rows, raw_out):
        shape = (out_rows, held * tiles) if raw_out else (held * tiles, out_rows)
        tall, flat = iota(shape, 1 if raw_out else 0), iota(shape, 0 if raw_out else 1)
        token, tile = tall % held, tall // held
        place = token // levels * (tiles * levels) + tile * levels + token % levels
        return jnp.where((place == flat) & (token < count), 1.0, 0.0).astype(BF16)

    rest = real - cut
    rest_held = rows - cut
    cuts = ((0, cut, cut, cut_rows), (cut, rest, rest_held, slab_rows - cut_rows))
    sorts, puts = (sort0, sort1), (put0, put1)
    for (_, count, held, n), pick, put in zip(cuts, sorts, puts):
        pick[...] = shuffle(count, held, n, False)
        put[...] = shuffle(count, held, n, True)

    last = jnp.where(a == na - 1, mine, 0)
    row_in_block = iota((pair_rows, lanes), 0) % rows
    valid = row_in_block < real
    raw_bias = jnp.zeros((1, lanes), F32)
    qscale = jnp.zeros((1, width), F32)
    for h in range(heads):
        raw_bias = jnp.where(
            iota((1, lanes), 1) // 2 == h, bias_ref[h] * LOG2E, raw_bias
        )
        qscale = jnp.where(
            iota((1, width), 1) // head_size == h, scale_ref[h] * (LOG2E / head_size), qscale
        )
    bias_hi = raw_bias.astype(BF16).astype(F32)
    bias_row = jnp.where(iota(raw_bias.shape, 1) % 2 == 0, bias_hi, raw_bias - bias_hi)
    span = 2 * lanes
    blocks[...] = jnp.where(
        iota((span, span), 0) // head_size == iota((span, span), 1) // head_size,
        1.0 / head_size, 0.0,
    ).astype(BF16)
    ones = jnp.where(valid, 1.0, 0.0).astype(BF16)

    def arrive(p):
        for cc in (0, 1):
            i = 2 * p + cc
            pltpu.make_async_copy(rin.at[i], rin.at[i], recv1.at[i]).wait()
        both = jnp.concatenate([rin[2 * p + cc].reshape(slab_rows, 128) for cc in (0, 1)], 1)
        start = 0
        for (token, _, held, n), pick in zip(cuts, sorts):
            tall = dot(pick[...], both[start : start + n]).astype(BF16)
            start += n
            for cc in (0, 1):
                for t in range(tiles):
                    win[p, cc, token : token + held, 128 * t : 128 * (t + 1)] = tall[
                        t * held : (t + 1) * held, 128 * cc : 128 * (cc + 1)
                    ]

    def mark(rr, carry):
        token = iota((rows, 1), 0)
        cell = token // levels
        lane = iota((rows, lanes), 1)
        late = (rr * last).astype(F32)
        far = jnp.where(
            lane == 2 * heads, FAR * late, jnp.where(lane == 2 * heads + 1, FAR * (1 - late), 0.0)
        )
        over = (rr * mine).astype(F32)
        for cc in (0, 1):
            near = tidy[...] if cc == 0 else marked[0]
            near = near + over * (marked[1 + cc] - near)
            at_lat = (SH_LAT * row_of(mine, rr) + cell // SH_LON % SH_LAT) * levels + token % levels
            at_lon = (1 - cc) * SH_LON + cell % SH_LON
            by_lat = jnp.where(iota((rows, tidy.shape[0]), 1) == at_lat, 1.0, 0.0).astype(BF16)
            by_cell = dot(by_lat, near.astype(BF16))
            by_cell = jnp.where(iota((rows, 128), 1) == at_lon, by_cell, 0.0).astype(BF16)
            marks = dot(by_cell, jnp.ones((128, lanes), BF16))
            key = (marks * bias_row + far).astype(BF16)
            for d in (0, 1):
                at = pl.multiple_of((2 * d + rr) * pair_rows + cc * rows, 16)
                kx[pl.ds(at, rows)] = key
        return carry

    def project(p):
        both = win[p].reshape(pair_rows, width)
        normed = layer_norm(both.astype(F32)).astype(BF16)
        here = pl.ds(pl.multiple_of(p * pair_rows, 16), pair_rows)
        spans = width // span

        def mix(part, s):
            lo = part * width + s * span
            return dot(normed, wqkv[:, lo : lo + span])

        def unify(part, s, mixed):
            square = dot((mixed * mixed).astype(BF16), blocks[...])
            unit = mixed * lax.rsqrt(square + 1e-06)
            if part == 0:
                unit = unit * qscale[:, s * span : (s + 1) * span]
            unit = unit.astype(BF16)
            store = ks if part else qs
            store[2 * s, here] = unit[:, :lanes]
            store[2 * s + 1, here] = unit[:, lanes:]

        def keep(s, mixed):
            for k in (0, 1):
                vs[2 * s + k, here] = jnp.where(
                    valid, mixed[:, k * lanes : (k + 1) * lanes], 0.0
                ).astype(BF16)

        jobs = [(part, s) for part in (0, 1) for s in range(spans)]
        waiting = []
        for part, s in jobs:
            waiting.append((part, s, mix(part, s)))
            if len(waiting) > 1:
                unify(*waiting.pop(0))
        for s in range(spans):
            mixed = mix(2, s)
            if waiting:
                unify(*waiting.pop(0))
            keep(s, mixed)

    q_lane = iota((pair_rows, lanes), 1)
    low = q_lane < head_size
    sides = [jnp.where(low if e == 0 else ~low, 1.0, 0.0).astype(BF16) for e in (0, 1)]
    ones_all = jnp.concatenate([ones, ones], 0)

    def attend(q, k0, sink):
        here = pl.ds(pl.multiple_of(q * pair_rows, 16), pair_rows)
        q_late = (q % 2 * last).astype(F32)
        q_region = jnp.where(
            q_lane == 2 * heads, 1 - q_late, jnp.where(q_lane == 2 * heads + 1, q_late, 0.0)
        )

        def weigh(pair):
            query = qs[pair, here]
            keys = jnp.concatenate([ks[pair, k0 : k0 + half], kx[k0 : k0 + half]], 1)
            asked = [
                jnp.concatenate(
                    [
                        query * sides[e],
                        jnp.where(q_lane // 2 == 2 * pair + e, 1.0, q_region).astype(BF16),
                    ],
                    1,
                )
                for e in (0, 1)
            ]
            soft[pair % 2] = jnp.exp2(dot_t(jnp.concatenate(asked, 0), keys)).astype(BF16)

        def gain(pair):
            values = jnp.concatenate([vs[pair, k0 : k0 + half], ones_all], 1)
            summed = dot(soft[pair % 2], values)
            up, down = summed[:pair_rows], summed[pair_rows:]
            sink(
                pair,
                jnp.where(low, up[:, :lanes], down[:, :lanes]),
                jnp.where(low, up[:, lanes:], down[:, lanes:]),
            )

        weigh(0)
        for pair in range(pairs):
            if pair + 1 < pairs:
                weigh(pair + 1)
            gain(pair)

    def attend_near(q, carry):
        def sink(pair, above, below):
            acc[q, pair, 0] = above
            acc[q, pair, 1] = below

        attend(q, 0, sink)
        return carry

    def attend_far(q):
        def sink(pair, above, below):
            ratio = (above + acc[q, pair, 0]) / (below + acc[q, pair, 1])
            att[:, pair * lanes : (pair + 1) * lanes] = ratio.astype(BF16)

        attend(q, half, sink)

    def join(p):
        projected = dot(att[...], wout[...]).astype(BF16)
        own = win[p].reshape(pair_rows, width)
        residual = (own.astype(F32) + projected.astype(F32)).astype(BF16).astype(F32)
        mlp_in = layer_norm(residual).astype(BF16)
        update = jnp.zeros_like(residual)
        hidden_size = wup.shape[1]
        piece = 512
        slope = math.sqrt(2.0 / math.pi)

        def raise_(s):
            up = dot(mlp_in, wup[:, s * piece : (s + 1) * piece])
            bent = jnp.tanh(up * (slope + 0.044715 * slope * (up * up)))
            return (up + up * bent).astype(BF16)

        pieces = hidden_size // piece
        twice = raise_(0)
        for s in range(pieces):
            later = raise_(s + 1) if s + 1 < pieces else None
            update = update + dot(twice, wdown[s * piece : (s + 1) * piece, :])
            twice = later
        joined = (residual + 0.5 * update).astype(BF16)
        flat = []
        for (token, _, held, _), put in zip(cuts, puts):
            tall = jnp.concatenate(
                [
                    jnp.concatenate(
                        [
                            joined[cc * rows + token : cc * rows + token + held, 128 * t : 128 * (t + 1)]
                            for t in range(tiles)
                        ],
                        0,
                    )
                    for cc in (0, 1)
                ],
                1,
            )
            flat.append(dot(put[...], tall).astype(BF16))
        flat = jnp.concatenate(flat, 0)
        d, rr = p // 2, p % 2
        for cc in (1, 0):
            rout[2 * p + cc] = flat[:, 128 * cc : 128 * (cc + 1)].reshape(slab)
            if cc == 1:
                backward(d, cc, rr).start()
            else:
                away = d + rr * mine
                pl.when(away > 0)(lambda: backward(d, 0, rr).start())
                pl.when(away == 0)(lambda: settle(0, rr).start())

    weights[0].wait()

    def gather(t, carry):
        arrive(t)
        project(t)
        first = jnp.where(t == 1, 0, t)
        lax.fori_loop(first, jnp.where(t == 0, 0, t + 1), attend_near, 0)
        return carry

    def scatter(t, carry):
        p = 3 - t
        attend_far(p)
        join(p)
        return carry

    for n in range(3):
        pltpu.make_async_copy(marked.at[n], marked.at[n], mrecv.at[n]).wait()
    lax.fori_loop(0, 2, mark, 0)
    lax.fori_loop(0, 4, gather, 0)
    for copy in weights[1:]:
        copy.wait()
    lax.fori_loop(0, 4, scatter, 0)

    for n in range(3):
        share(n).wait_send()
    for d, cc, rr in order:
        by_owner(d, cc, rr, None, lambda: forward(d, cc, rr).wait_send())
    for d, cc, rr in order:
        by_owner(d, cc, rr, None, lambda: backward(d, cc, rr).wait_send())
    for d, cc, rr in order:
        landed = block_of(out_ref, (g + b + d + cc) % 2, cc, rr)
        pltpu.make_async_copy(landed, landed, recv2.at[4 * d + 2 * rr + cc]).wait()


def hand_over(src, dst, sem):
    gives = [pltpu.make_async_copy(src.at[i], dst.at[i], sem.at[i]) for i in range(src.shape[0])]
    for give in gives:
        give.start()
    for give in gives:
        give.wait()


def per_device(fields, surface_mask, w_qkv, w_out, logit_scale, mask_bias, w_up, w_down):
    groups, levels, nlat, nlon, width = fields.shape
    heads = logit_scale.shape[0]
    head_size = width // heads
    real = groups * levels * SH_LAT * SH_LON
    rows = -(-real // 16) * 16
    total = 8 * rows

    tiles = width // 128
    raw = fields.reshape(groups, levels, nlat, nlon, tiles, 128)
    raw = jnp.transpose(raw, (0, 2, 3, 4, 1, 5))
    raw = raw.reshape(groups, nlat, nlon // 2, 2 * tiles * levels, 128)
    slab = (groups, SH_LAT, SH_LON // 2) + raw.shape[3:]

    cut = 256 // tiles
    spans = ((256, cut * tiles), (math.prod(slab[:-1]) - 256, (rows - cut) * tiles))
    orders = [(held, flat) for flat, held in spans] + list(spans)

    vmem = pl.BlockSpec(memory_space=pltpu.VMEM)
    anywhere = pl.BlockSpec(memory_space=pl.ANY)
    joined = pl.pallas_call(
        functools.partial(kernel, real, heads),
        out_shape=pltpu.VMEM(raw.shape, BF16),
        in_specs=[anywhere] * 8,
        out_specs=anywhere,
        scratch_shapes=[
            pltpu.VMEM(raw.shape, BF16),
            pltpu.VMEM((nlat, levels, nlon), jnp.int32),
            pltpu.SMEM(logit_scale.shape, F32),
            pltpu.SMEM(mask_bias.shape, F32),
            pltpu.VMEM((nlat * levels, 128), F32),
            pltpu.VMEM((3, nlat * levels, 128), F32),
            pltpu.VMEM((8,) + slab, BF16),
            pltpu.VMEM((4, 2, rows, width), BF16),
            pltpu.VMEM(w_qkv.shape, BF16),
            pltpu.VMEM(w_out.shape, BF16),
            pltpu.VMEM(w_up.shape, BF16),
            pltpu.VMEM(w_down.shape, BF16),
            pltpu.VMEM((total // 4, width), BF16),
            pltpu.VMEM((heads // 2, total, 2 * head_size), BF16),
            pltpu.VMEM((heads // 2, total, 2 * head_size), BF16),
            pltpu.VMEM((heads // 2, total, 2 * head_size), BF16),
            pltpu.VMEM((total, 2 * head_size), BF16),
            pltpu.VMEM((4, heads // 2, 2, total // 4, 2 * head_size), F32),
            pltpu.VMEM((8,) + slab, BF16),
        ]
        + [pltpu.VMEM(shape, BF16) for shape in orders]
        + [
            pltpu.VMEM((4 * head_size, 4 * head_size), BF16),
            pltpu.VMEM((2, total // 2, total // 2), BF16),
            pltpu.SemaphoreType.DMA((5,)),
            pltpu.SemaphoreType.DMA((3,)),
            pltpu.SemaphoreType.DMA((3,)),
            pltpu.SemaphoreType.DMA((3,)),
            pltpu.SemaphoreType.DMA((8,)),
            pltpu.SemaphoreType.DMA((8,)),
            pltpu.SemaphoreType.DMA((8,)),
            pltpu.SemaphoreType.DMA((8,)),
        ],
        compiler_params=pltpu.CompilerParams(
            collective_id=0, has_side_effects=True, vmem_limit_bytes=56 * 1024 * 1024
        ),
        name="window_block",
    )(raw, jnp.transpose(surface_mask, (1, 0, 2)), logit_scale, mask_bias, w_qkv, w_out, w_up, w_down)

    joined = pl.pallas_call(
        hand_over,
        out_shape=jax.ShapeDtypeStruct(raw.shape, BF16),
        in_specs=[vmem],
        out_specs=anywhere,
        scratch_shapes=[pltpu.SemaphoreType.DMA((groups,))],
        name="hand_over",
    )(pltpu.with_memory_space_constraint(joined, pltpu.VMEM))
    joined = joined.reshape(groups, nlat, nlon, tiles, levels, 128)
    return jnp.transpose(joined, (0, 4, 1, 2, 3, 5)).reshape(fields.shape)


def solution(mesh):
    return jax.shard_map(
        per_device,
        mesh=mesh,
        in_specs=(
            P("grp", None, "lat", "lon", None),
            P(None, "lat", "lon"),
            P(),
            P(),
            P(),
            P(),
            P(),
            P(),
        ),
        out_specs=P("grp", None, "lat", "lon", None),
        check_vma=False,
    )
```

```python
import functools
import math

import jax
import jax.numpy as jnp
from jax import lax
from jax.experimental import pallas as pl
from jax.experimental.pallas import tpu as pltpu
from jax.sharding import PartitionSpec as P

SH_LAT = 3
SH_LON = 6
LOG2E = math.log2(math.e)
FAR = -30000.0
MESH = pl.DeviceIdType.MESH
BF16 = jnp.bfloat16
F32 = jnp.float32


def layer_norm(values):
    centred = values - jnp.mean(values, -1, keepdims=True)
    return centred * lax.rsqrt(jnp.mean(centred * centred, -1, keepdims=True) + 1e-05)


def iota(shape, axis):
    return lax.broadcasted_iota(jnp.int32, shape, axis)


def dot(left, right):
    return jnp.dot(left, right, preferred_element_type=F32)


def dot_t(left, right):
    return lax.dot_general(left, right, (((1,), (1,)), ((), ())), preferred_element_type=F32)


def kernel(
    real, heads,
    fields_hbm, mask_hbm, scale_hbm, bias_hbm, wqkv_hbm, wout_hbm, wup_hbm, wdown_hbm,
    out_ref,
    raw, mask_ref, scale_ref, bias_ref, tidy, marked, rin, win, wqkv, wout, wup, wdown, att, qs, ks, vs,
    kx, acc, rout, sort0, sort1, put0, put1, blocks, soft,
    wsem, ssem, msend, mrecv, send1, recv1, send2, recv2,
):
    rows, width = win.shape[2:]
    levels = mask_ref.shape[1]
    nlat = mask_ref.shape[0]
    tiles = width // 128
    side_pairs = SH_LON // 2
    slab = rin.shape[1:]
    slab_rows = slab[0] * slab[1] * slab[2] * slab[3]
    pair_rows = 2 * rows
    half = 2 * pair_rows
    total = 2 * half
    pairs = heads // 2
    head_size = width // heads
    lanes = 2 * head_size
    cut_rows = 256
    cut = cut_rows // tiles

    g, a, b = lax.axis_index("grp"), lax.axis_index("lat"), lax.axis_index("lon")
    na, nb = lax.axis_size("lat"), lax.axis_size("lon")
    mine = (g + b) % 2

    def peer(d, da, db):
        return {"grp": (g + d) % 2, "lat": (a + da + na) % na, "lon": (b + db + nb) % nb}

    barrier = pltpu.get_barrier_semaphore()
    greeted = 0
    for d in (0, 1):
        for da, db in ((0, 0), (-1, 0), (0, -1), (-1, -1), (1, 0), (0, 1), (1, 1)):
            if d or da or db:
                pl.semaphore_signal(barrier, inc=1, device_id=peer(d, da, db), device_id_type=MESH)
                greeted += 1

    last = jnp.where(a == na - 1, mine, 0)

    def slot(d, cc, rr, crossed):
        same = 1 - (1 - d) * crossed
        return 4 * d + 2 * (rr + same * (cc - rr)) + cc + same * (rr - cc)

    def row_of(parity, rr):
        return (1 + 2 * parity + rr) % 4

    def block_of(ref, parity, cc, rr):
        r = row_of(parity, rr)
        return ref.at[:, pl.ds(SH_LAT * r, SH_LAT), pl.ds(side_pairs * (1 - cc), side_pairs)]

    def by_owner(d, cc, rr, local, remote):
        if d or cc:
            remote()
        elif rr == 0:
            if local is not None:
                local()
        else:
            pl.when(mine == 1)(remote)
            if local is not None:
                pl.when(mine == 0)(local)

    def stay(cc, rr):
        i = slot(0, cc, rr, 0)
        return pltpu.make_async_copy(block_of(fields_hbm, mine, cc, rr), rin.at[i], recv1.at[i])

    def forward(d, cc, rr):
        n = 4 * d + 2 * cc + rr
        parity = (g + b + d + cc) % 2
        i = slot(d, cc, rr, jnp.where((a - rr * parity + na) % na == na - 1, parity, 0))
        return pltpu.make_async_remote_copy(
            src_ref=block_of(raw, parity, cc, rr), dst_ref=rin.at[i],
            send_sem=send1.at[n], recv_sem=recv1.at[i],
            device_id=peer(d, -rr * parity, -cc), device_id_type=MESH,
        )

    def backward(d, cc, rr):
        n = 4 * d + 2 * cc + rr
        return pltpu.make_async_remote_copy(
            src_ref=rout.at[slot(d, cc, rr, last)], dst_ref=block_of(out_ref, mine, cc, rr),
            send_sem=send2.at[n], recv_sem=recv2.at[n],
            device_id=peer(d, rr * mine, cc), device_id_type=MESH,
        )

    def settle(cc, rr):
        n = 2 * cc + rr
        return pltpu.make_async_copy(
            rout.at[slot(0, cc, rr, last)], block_of(out_ref, mine, cc, rr), recv2.at[n]
        )

    def share(n):
        da, db = ((0, -1), (-1, 0), (-1, -1))[n]
        return pltpu.make_async_remote_copy(
            src_ref=tidy, dst_ref=marked.at[n], send_sem=msend.at[n], recv_sem=mrecv.at[n],
            device_id=peer(0, da, db), device_id_type=MESH,
        )

    load = pltpu.make_async_copy(fields_hbm, raw, wsem.at[4])
    load.start()
    small = [
        pltpu.make_async_copy(src, dst, ssem.at[i])
        for i, (src, dst) in enumerate(
            ((mask_hbm, mask_ref), (scale_hbm, scale_ref), (bias_hbm, bias_ref))
        )
    ]
    for copy in small:
        copy.start()
    stay(0, 0).start()
    pl.when(mine == 0)(lambda: stay(0, 1).start())
    weights = [
        pltpu.make_async_copy(src, dst, wsem.at[i])
        for i, (src, dst) in enumerate(
            ((wqkv_hbm, wqkv), (wout_hbm, wout), (wup_hbm, wup), (wdown_hbm, wdown))
        )
    ]

    for copy in small:
        copy.wait()
    tidy[...] = jnp.zeros_like(tidy)
    for i in range(nlat):
        tidy[levels * i : levels * (i + 1), : mask_ref.shape[2]] = mask_ref[i].astype(F32)

    load.wait()
    for copy in weights:
        copy.start()
    pl.semaphore_wait(barrier, greeted)
    for n in range(3):
        share(n).start()
    order = [(0, cc, rr) for rr in (0, 1) for cc in (1, 0)]
    order += [(1, cc, rr) for cc in (0, 1) for rr in (0, 1)]
    for d, cc, rr in order:
        by_owner(d, cc, rr, None, lambda: forward(d, cc, rr).start())

    def shuffle(count, held, out_rows, raw_out):
        shape = (out_rows, held * tiles) if raw_out else (held * tiles, out_rows)
        tall, flat = iota(shape, 1 if raw_out else 0), iota(shape, 0 if raw_out else 1)
        token, tile = tall % held, tall // held
        place = token // levels * (tiles * levels) + tile * levels + token % levels
        return jnp.where((place == flat) & (token < count), 1.0, 0.0).astype(BF16)

    rest = real - cut
    rest_held = rows - cut
    cuts = ((0, cut, cut, cut_rows), (cut, rest, rest_held, slab_rows - cut_rows))
    sorts, puts = (sort0, sort1), (put0, put1)
    for (_, count, held, n), pick, put in zip(cuts, sorts, puts):
        pick[...] = shuffle(count, held, n, False)
        put[...] = shuffle(count, held, n, True)

    row_in_block = iota((pair_rows, lanes), 0) % rows
    valid = row_in_block < real
    raw_bias = jnp.zeros((1, lanes), F32)
    qscale = jnp.zeros((1, width), F32)
    for h in range(heads):
        raw_bias = jnp.where(
            iota((1, lanes), 1) // 2 == h, bias_ref[h] * LOG2E, raw_bias
        )
        qscale = jnp.where(
            iota((1, width), 1) // head_size == h, scale_ref[h] * (LOG2E / head_size), qscale
        )
    bias_hi = raw_bias.astype(BF16).astype(F32)
    bias_row = jnp.where(iota(raw_bias.shape, 1) % 2 == 0, bias_hi, raw_bias - bias_hi)
    span = 2 * lanes
    blocks[...] = jnp.where(
        iota((span, span), 0) // head_size == iota((span, span), 1) // head_size,
        1.0 / head_size, 0.0,
    ).astype(BF16)
    ones = jnp.where(valid, 1.0, 0.0).astype(BF16)

    def arrive(p):
        for rr in (0, 1):
            i = 2 * p + rr
            pltpu.make_async_copy(rin.at[i], rin.at[i], recv1.at[i]).wait()
        both = jnp.concatenate([rin[2 * p + rr].reshape(slab_rows, 128) for rr in (0, 1)], 1)
        start = 0
        for (token, _, held, n), pick in zip(cuts, sorts):
            tall = dot(pick[...], both[start : start + n]).astype(BF16)
            start += n
            for rr in (0, 1):
                for t in range(tiles):
                    win[p, rr, token : token + held, 128 * t : 128 * (t + 1)] = tall[
                        t * held : (t + 1) * held, 128 * rr : 128 * (rr + 1)
                    ]

    def mark(rr, carry):
        token = iota((rows, 1), 0)
        cell = token // levels
        lane = iota((rows, lanes), 1)
        late = (rr * last).astype(F32)
        far = jnp.where(
            lane == 2 * heads, FAR * late, jnp.where(lane == 2 * heads + 1, FAR * (1 - late), 0.0)
        )
        over = (rr * mine).astype(F32)
        for cc in (0, 1):
            near = tidy[...] if cc == 0 else marked[0]
            near = near + over * (marked[1 + cc] - near)
            at_lat = (SH_LAT * row_of(mine, rr) + cell // SH_LON % SH_LAT) * levels + token % levels
            at_lon = (1 - cc) * SH_LON + cell % SH_LON
            by_lat = jnp.where(iota((rows, tidy.shape[0]), 1) == at_lat, 1.0, 0.0).astype(BF16)
            by_cell = dot(by_lat, near.astype(BF16))
            by_cell = jnp.where(iota((rows, 128), 1) == at_lon, by_cell, 0.0).astype(BF16)
            marks = dot(by_cell, jnp.ones((128, lanes), BF16))
            key = (marks * bias_row + far).astype(BF16)
            for d in (0, 1):
                at = pl.multiple_of(slot(d, cc, rr, last) * rows, 16)
                kx[pl.ds(at, rows)] = key
        return carry

    def project(p):
        both = win[p].reshape(pair_rows, width)
        normed = layer_norm(both.astype(F32)).astype(BF16)
        here = pl.ds(pl.multiple_of(p * pair_rows, 16), pair_rows)
        spans = width // span

        def mix(part, s):
            lo = part * width + s * span
            return dot(normed, wqkv[:, lo : lo + span])

        def unify(part, s, mixed):
            square = dot((mixed * mixed).astype(BF16), blocks[...])
            unit = mixed * lax.rsqrt(square + 1e-06)
            if part == 0:
                unit = unit * qscale[:, s * span : (s + 1) * span]
            unit = unit.astype(BF16)
            store = ks if part else qs
            store[2 * s, here] = unit[:, :lanes]
            store[2 * s + 1, here] = unit[:, lanes:]

        def keep(s, mixed):
            for k in (0, 1):
                vs[2 * s + k, here] = jnp.where(
                    valid, mixed[:, k * lanes : (k + 1) * lanes], 0.0
                ).astype(BF16)

        jobs = [(part, s) for part in (0, 1) for s in range(spans)]
        waiting = []
        for part, s in jobs:
            waiting.append((part, s, mix(part, s)))
            if len(waiting) > 1:
                unify(*waiting.pop(0))
        for s in range(spans):
            mixed = mix(2, s)
            if waiting:
                unify(*waiting.pop(0))
            keep(s, mixed)

    q_lane = iota((pair_rows, lanes), 1)
    low = q_lane < head_size
    lower = jnp.where(iota((pair_rows, lanes), 0) >= rows, 1, 0)
    sides = [jnp.where(low if e == 0 else ~low, 1.0, 0.0).astype(BF16) for e in (0, 1)]
    ones_all = jnp.concatenate([ones, ones], 0)

    def attend(q, k0, sink):
        here = pl.ds(pl.multiple_of(q * pair_rows, 16), pair_rows)
        q_late = (last * (q % 2 + q // 2 * (lower - q % 2))).astype(F32)
        q_region = jnp.where(
            q_lane == 2 * heads, 1 - q_late, jnp.where(q_lane == 2 * heads + 1, q_late, 0.0)
        )

        def weigh(pair):
            query = qs[pair, here]
            keys = jnp.concatenate([ks[pair, k0 : k0 + half], kx[k0 : k0 + half]], 1)
            asked = [
                jnp.concatenate(
                    [
                        query * sides[e],
                        jnp.where(q_lane // 2 == 2 * pair + e, 1.0, q_region).astype(BF16),
                    ],
                    1,
                )
                for e in (0, 1)
            ]
            soft[pair % 2] = jnp.exp2(dot_t(jnp.concatenate(asked, 0), keys)).astype(BF16)

        def gain(pair):
            values = jnp.concatenate([vs[pair, k0 : k0 + half], ones_all], 1)
            summed = dot(soft[pair % 2], values)
            up, down = summed[:pair_rows], summed[pair_rows:]
            sink(
                pair,
                jnp.where(low, up[:, :lanes], down[:, :lanes]),
                jnp.where(low, up[:, lanes:], down[:, lanes:]),
            )

        weigh(0)
        for pair in range(pairs):
            if pair + 1 < pairs:
                weigh(pair + 1)
            gain(pair)

    def attend_near(q, carry):
        def sink(pair, above, below):
            acc[q, pair, 0] = above
            acc[q, pair, 1] = below

        attend(q, 0, sink)
        return carry

    def attend_far(q):
        def sink(pair, above, below):
            ratio = (above + acc[q, pair, 0]) / (below + acc[q, pair, 1])
            att[:, pair * lanes : (pair + 1) * lanes] = ratio.astype(BF16)

        attend(q, half, sink)

    def join(p):
        projected = dot(att[...], wout[...]).astype(BF16)
        own = win[p].reshape(pair_rows, width)
        residual = (own.astype(F32) + projected.astype(F32)).astype(BF16).astype(F32)
        mlp_in = layer_norm(residual).astype(BF16)
        update = jnp.zeros_like(residual)
        hidden_size = wup.shape[1]
        piece = 512
        slope = math.sqrt(2.0 / math.pi)

        def raise_(s):
            up = dot(mlp_in, wup[:, s * piece : (s + 1) * piece])
            bent = jnp.tanh(up * (slope + 0.044715 * slope * (up * up)))
            return (up + up * bent).astype(BF16)

        pieces = hidden_size // piece
        twice = raise_(0)
        for s in range(pieces):
            later = raise_(s + 1) if s + 1 < pieces else None
            update = update + dot(twice, wdown[s * piece : (s + 1) * piece, :])
            twice = later
        joined = (residual + 0.5 * update).astype(BF16)
        flat = []
        for (token, _, held, _), put in zip(cuts, puts):
            tall = jnp.concatenate(
                [
                    jnp.concatenate(
                        [
                            joined[rr * rows + token : rr * rows + token + held, 128 * t : 128 * (t + 1)]
                            for t in range(tiles)
                        ],
                        0,
                    )
                    for rr in (0, 1)
                ],
                1,
            )
            flat.append(dot(put[...], tall).astype(BF16))
        flat = jnp.concatenate(flat, 0)
        d, other = p // 2, p % 2
        for k in (1, 0):
            rout[2 * p + k] = flat[:, 128 * k : 128 * (k + 1)].reshape(slab)
            same = 1 - (1 - d) * last
            cc, rr = k + same * (other - k), other + same * (k - other)
            away = d + cc + rr * mine
            pl.when(away > 0)(lambda: backward(d, cc, rr).start())
            pl.when(away == 0)(lambda: settle(cc, rr).start())

    weights[0].wait()

    def mark_all():
        for n in range(3):
            pltpu.make_async_copy(marked.at[n], marked.at[n], mrecv.at[n]).wait()
        lax.fori_loop(0, 2, mark, 0)

    def gather(t, carry):
        arrive(t)
        project(t)
        pl.when(t == 1)(mark_all)
        first = jnp.where(t == 1, 0, t)
        lax.fori_loop(first, jnp.where(t == 0, 0, t + 1), attend_near, 0)
        return carry

    def scatter(t, carry):
        p = 3 - t
        attend_far(p)
        join(p)
        return carry

    lax.fori_loop(0, 4, gather, 0)
    for copy in weights[1:]:
        copy.wait()
    lax.fori_loop(0, 4, scatter, 0)

    for n in range(3):
        share(n).wait_send()
    for d, cc, rr in order:
        by_owner(d, cc, rr, None, lambda: forward(d, cc, rr).wait_send())
    for d, cc, rr in order:
        by_owner(d, cc, rr, None, lambda: backward(d, cc, rr).wait_send())
    for d, cc, rr in order:
        landed = block_of(out_ref, (g + b + d + cc) % 2, cc, rr)
        pltpu.make_async_copy(landed, landed, recv2.at[4 * d + 2 * cc + rr]).wait()


def hand_over(src, dst, sem):
    gives = [pltpu.make_async_copy(src.at[i], dst.at[i], sem.at[i]) for i in range(src.shape[0])]
    for give in gives:
        give.start()
    for give in gives:
        give.wait()


def per_device(fields, surface_mask, w_qkv, w_out, logit_scale, mask_bias, w_up, w_down):
    groups, levels, nlat, nlon, width = fields.shape
    heads = logit_scale.shape[0]
    head_size = width // heads
    real = groups * levels * SH_LAT * SH_LON
    rows = -(-real // 16) * 16
    total = 8 * rows

    tiles = width // 128
    raw = fields.reshape(groups, levels, nlat, nlon, tiles, 128)
    raw = jnp.transpose(raw, (0, 2, 3, 4, 1, 5))
    raw = raw.reshape(groups, nlat, nlon // 2, 2 * tiles * levels, 128)
    slab = (groups, SH_LAT, SH_LON // 2) + raw.shape[3:]

    cut = 256 // tiles
    spans = ((256, cut * tiles), (math.prod(slab[:-1]) - 256, (rows - cut) * tiles))
    orders = [(held, flat) for flat, held in spans] + list(spans)

    vmem = pl.BlockSpec(memory_space=pltpu.VMEM)
    anywhere = pl.BlockSpec(memory_space=pl.ANY)
    joined = pl.pallas_call(
        functools.partial(kernel, real, heads),
        out_shape=pltpu.VMEM(raw.shape, BF16),
        in_specs=[anywhere] * 8,
        out_specs=anywhere,
        scratch_shapes=[
            pltpu.VMEM(raw.shape, BF16),
            pltpu.VMEM((nlat, levels, nlon), jnp.int32),
            pltpu.SMEM(logit_scale.shape, F32),
            pltpu.SMEM(mask_bias.shape, F32),
            pltpu.VMEM((nlat * levels, 128), F32),
            pltpu.VMEM((3, nlat * levels, 128), F32),
            pltpu.VMEM((8,) + slab, BF16),
            pltpu.VMEM((4, 2, rows, width), BF16),
            pltpu.VMEM(w_qkv.shape, BF16),
            pltpu.VMEM(w_out.shape, BF16),
            pltpu.VMEM(w_up.shape, BF16),
            pltpu.VMEM(w_down.shape, BF16),
            pltpu.VMEM((total // 4, width), BF16),
            pltpu.VMEM((heads // 2, total, 2 * head_size), BF16),
            pltpu.VMEM((heads // 2, total, 2 * head_size), BF16),
            pltpu.VMEM((heads // 2, total, 2 * head_size), BF16),
            pltpu.VMEM((total, 2 * head_size), BF16),
            pltpu.VMEM((4, heads // 2, 2, total // 4, 2 * head_size), F32),
            pltpu.VMEM((8,) + slab, BF16),
        ]
        + [pltpu.VMEM(shape, BF16) for shape in orders]
        + [
            pltpu.VMEM((4 * head_size, 4 * head_size), BF16),
            pltpu.VMEM((2, total // 2, total // 2), BF16),
            pltpu.SemaphoreType.DMA((5,)),
            pltpu.SemaphoreType.DMA((3,)),
            pltpu.SemaphoreType.DMA((3,)),
            pltpu.SemaphoreType.DMA((3,)),
            pltpu.SemaphoreType.DMA((8,)),
            pltpu.SemaphoreType.DMA((8,)),
            pltpu.SemaphoreType.DMA((8,)),
            pltpu.SemaphoreType.DMA((8,)),
        ],
        compiler_params=pltpu.CompilerParams(
            collective_id=0, has_side_effects=True, vmem_limit_bytes=56 * 1024 * 1024
        ),
        name="window_block",
    )(raw, jnp.transpose(surface_mask, (1, 0, 2)), logit_scale, mask_bias, w_qkv, w_out, w_up, w_down)

    joined = pl.pallas_call(
        hand_over,
        out_shape=jax.ShapeDtypeStruct(raw.shape, BF16),
        in_specs=[vmem],
        out_specs=anywhere,
        scratch_shapes=[pltpu.SemaphoreType.DMA((groups,))],
        name="hand_over",
    )(pltpu.with_memory_space_constraint(joined, pltpu.VMEM))
    joined = joined.reshape(groups, nlat, nlon, tiles, levels, 128)
    return jnp.transpose(joined, (0, 4, 1, 2, 3, 5)).reshape(fields.shape)


def solution(mesh):
    return jax.shard_map(
        per_device,
        mesh=mesh,
        in_specs=(
            P("grp", None, "lat", "lon", None),
            P(None, "lat", "lon"),
            P(),
            P(),
            P(),
            P(),
            P(),
            P(),
        ),
        out_specs=P("grp", None, "lat", "lon", None),
        check_vma=False,
    )
```

```python
import functools
import math

import jax
import jax.numpy as jnp
from jax import lax
from jax.experimental import pallas as pl
from jax.experimental.pallas import tpu as pltpu
from jax.sharding import PartitionSpec as P

SH_LAT = 3
SH_LON = 6
LOG2E = math.log2(math.e)
FAR = -30000.0
MESH = pl.DeviceIdType.MESH
BF16 = jnp.bfloat16
F32 = jnp.float32


def layer_norm(values):
    centred = values - jnp.mean(values, -1, keepdims=True)
    return centred * lax.rsqrt(jnp.mean(centred * centred, -1, keepdims=True) + 1e-05)


def iota(shape, axis):
    return lax.broadcasted_iota(jnp.int32, shape, axis)


def dot(left, right):
    return jnp.dot(left, right, preferred_element_type=F32)


def dot_t(left, right):
    return lax.dot_general(left, right, (((1,), (1,)), ((), ())), preferred_element_type=F32)


def kernel(
    real, heads,
    fields_hbm, mask_hbm, scale_hbm, bias_hbm, wqkv_hbm, wout_hbm, wup_hbm, wdown_hbm,
    out_ref,
    raw, mask_ref, scale_ref, bias_ref, tidy, marked, rin, win, wqkv, wout, wup, wdown, att, qs, ks, vs,
    kx, acc, rout, sort0, sort1, put0, put1, blocks, soft,
    wsem, ssem, msend, mrecv, send1, recv1, send2, recv2,
):
    rows, width = win.shape[2:]
    levels = mask_ref.shape[1]
    nlat = mask_ref.shape[0]
    tiles = width // 128
    side_pairs = SH_LON // 2
    slab = rin.shape[1:]
    slab_rows = slab[0] * slab[1] * slab[2] * slab[3]
    pair_rows = 2 * rows
    half = 2 * pair_rows
    total = 2 * half
    pairs = heads // 2
    head_size = width // heads
    lanes = 2 * head_size
    cut_rows = 256
    cut = cut_rows // tiles

    g, a, b = lax.axis_index("grp"), lax.axis_index("lat"), lax.axis_index("lon")
    na, nb = lax.axis_size("lat"), lax.axis_size("lon")
    mine = (g + b) % 2

    def peer(d, da, db):
        return {"grp": (g + d) % 2, "lat": (a + da + na) % na, "lon": (b + db + nb) % nb}

    barrier = pltpu.get_barrier_semaphore()
    greeted = 0
    for d in (0, 1):
        for da, db in ((0, 0), (-1, 0), (0, -1), (-1, -1), (1, 0), (0, 1), (1, 1)):
            if d or da or db:
                pl.semaphore_signal(barrier, inc=1, device_id=peer(d, da, db), device_id_type=MESH)
                greeted += 1

    last = jnp.where(a == na - 1, mine, 0)

    def slot(d, cc, rr, crossed):
        same = 1 - crossed
        return 4 * d + 2 * (rr + same * (cc - rr)) + cc + same * (rr - cc)

    def row_of(parity, rr):
        return (1 + 2 * parity + rr) % 4

    def block_of(ref, parity, cc, rr):
        r = row_of(parity, rr)
        return ref.at[:, pl.ds(SH_LAT * r, SH_LAT), pl.ds(side_pairs * (1 - cc), side_pairs)]

    def by_owner(d, cc, rr, local, remote):
        if d or cc:
            remote()
        elif rr == 0:
            if local is not None:
                local()
        else:
            pl.when(mine == 1)(remote)
            if local is not None:
                pl.when(mine == 0)(local)

    def stay(cc, rr):
        i = slot(0, cc, rr, 0)
        return pltpu.make_async_copy(block_of(fields_hbm, mine, cc, rr), rin.at[i], recv1.at[i])

    def forward(d, cc, rr):
        n = 4 * d + 2 * cc + rr
        parity = (g + b + d + cc) % 2
        i = slot(d, cc, rr, jnp.where((a - rr * parity + na) % na == na - 1, parity, 0))
        return pltpu.make_async_remote_copy(
            src_ref=block_of(raw, parity, cc, rr), dst_ref=rin.at[i],
            send_sem=send1.at[n], recv_sem=recv1.at[i],
            device_id=peer(d, -rr * parity, -cc), device_id_type=MESH,
        )

    def backward(d, cc, rr):
        n = 4 * d + 2 * cc + rr
        return pltpu.make_async_remote_copy(
            src_ref=rout.at[slot(d, cc, rr, last)], dst_ref=block_of(out_ref, mine, cc, rr),
            send_sem=send2.at[n], recv_sem=recv2.at[n],
            device_id=peer(d, rr * mine, cc), device_id_type=MESH,
        )

    def settle(cc, rr):
        n = 2 * cc + rr
        return pltpu.make_async_copy(
            rout.at[slot(0, cc, rr, last)], block_of(out_ref, mine, cc, rr), recv2.at[n]
        )

    def share(n):
        da, db = ((0, -1), (-1, 0), (-1, -1))[n]
        return pltpu.make_async_remote_copy(
            src_ref=tidy, dst_ref=marked.at[n], send_sem=msend.at[n], recv_sem=mrecv.at[n],
            device_id=peer(0, da, db), device_id_type=MESH,
        )

    load = pltpu.make_async_copy(fields_hbm, raw, wsem.at[4])
    load.start()
    small = [
        pltpu.make_async_copy(src, dst, ssem.at[i])
        for i, (src, dst) in enumerate(
            ((mask_hbm, mask_ref), (scale_hbm, scale_ref), (bias_hbm, bias_ref))
        )
    ]
    for copy in small:
        copy.start()
    stay(0, 0).start()
    pl.when(mine == 0)(lambda: stay(0, 1).start())
    weights = [
        pltpu.make_async_copy(src, dst, wsem.at[i])
        for i, (src, dst) in enumerate(
            ((wqkv_hbm, wqkv), (wout_hbm, wout), (wup_hbm, wup), (wdown_hbm, wdown))
        )
    ]

    for copy in small:
        copy.wait()
    tidy[...] = jnp.zeros_like(tidy)
    for i in range(nlat):
        tidy[levels * i : levels * (i + 1), : mask_ref.shape[2]] = mask_ref[i].astype(F32)

    load.wait()
    for copy in weights:
        copy.start()
    pl.semaphore_wait(barrier, greeted)
    for n in range(3):
        share(n).start()
    order = [(0, cc, rr) for rr in (0, 1) for cc in (1, 0)]
    order += [(1, cc, rr) for cc in (0, 1) for rr in (0, 1)]
    for d, cc, rr in order:
        by_owner(d, cc, rr, None, lambda: forward(d, cc, rr).start())

    def shuffle(count, held, out_rows, raw_out):
        shape = (out_rows, held * tiles) if raw_out else (held * tiles, out_rows)
        tall, flat = iota(shape, 1 if raw_out else 0), iota(shape, 0 if raw_out else 1)
        token, tile = tall % held, tall // held
        place = token // levels * (tiles * levels) + tile * levels + token % levels
        return jnp.where((place == flat) & (token < count), 1.0, 0.0).astype(BF16)

    rest = real - cut
    rest_held = rows - cut
    cuts = ((0, cut, cut, cut_rows), (cut, rest, rest_held, slab_rows - cut_rows))
    sorts, puts = (sort0, sort1), (put0, put1)
    for (_, count, held, n), pick, put in zip(cuts, sorts, puts):
        pick[...] = shuffle(count, held, n, False)
        put[...] = shuffle(count, held, n, True)

    row_in_block = iota((pair_rows, lanes), 0) % rows
    valid = row_in_block < real
    raw_bias = jnp.zeros((1, lanes), F32)
    qscale = jnp.zeros((1, width), F32)
    for h in range(heads):
        raw_bias = jnp.where(
            iota((1, lanes), 1) // 2 == h, bias_ref[h] * LOG2E, raw_bias
        )
        qscale = jnp.where(
            iota((1, width), 1) // head_size == h, scale_ref[h] * (LOG2E / head_size), qscale
        )
    bias_hi = raw_bias.astype(BF16).astype(F32)
    bias_row = jnp.where(iota(raw_bias.shape, 1) % 2 == 0, bias_hi, raw_bias - bias_hi)
    span = 2 * lanes
    blocks[...] = jnp.where(
        iota((span, span), 0) // head_size == iota((span, span), 1) // head_size,
        1.0 / head_size, 0.0,
    ).astype(BF16)
    ones = jnp.where(valid, 1.0, 0.0).astype(BF16)

    def arrive(p):
        for rr in (0, 1):
            i = 2 * p + rr
            pltpu.make_async_copy(rin.at[i], rin.at[i], recv1.at[i]).wait()
        both = jnp.concatenate([rin[2 * p + rr].reshape(slab_rows, 128) for rr in (0, 1)], 1)
        start = 0
        for (token, _, held, n), pick in zip(cuts, sorts):
            tall = dot(pick[...], both[start : start + n]).astype(BF16)
            start += n
            for rr in (0, 1):
                for t in range(tiles):
                    win[p, rr, token : token + held, 128 * t : 128 * (t + 1)] = tall[
                        t * held : (t + 1) * held, 128 * rr : 128 * (rr + 1)
                    ]

    def mark(rr, carry):
        token = iota((rows, 1), 0)
        cell = token // levels
        lane = iota((rows, lanes), 1)
        late = (rr * last).astype(F32)
        far = jnp.where(
            lane == 2 * heads, FAR * late, jnp.where(lane == 2 * heads + 1, FAR * (1 - late), 0.0)
        )
        over = (rr * mine).astype(F32)
        for cc in (0, 1):
            near = tidy[...] if cc == 0 else marked[0]
            near = near + over * (marked[1 + cc] - near)
            at_lat = (SH_LAT * row_of(mine, rr) + cell // SH_LON % SH_LAT) * levels + token % levels
            at_lon = (1 - cc) * SH_LON + cell % SH_LON
            by_lat = jnp.where(iota((rows, tidy.shape[0]), 1) == at_lat, 1.0, 0.0).astype(BF16)
            by_cell = dot(by_lat, near.astype(BF16))
            by_cell = jnp.where(iota((rows, 128), 1) == at_lon, by_cell, 0.0).astype(BF16)
            marks = dot(by_cell, jnp.ones((128, lanes), BF16))
            key = (marks * bias_row + far).astype(BF16)
            for d in (0, 1):
                at = pl.multiple_of(slot(d, cc, rr, last) * rows, 16)
                kx[pl.ds(at, rows)] = key
        return carry

    def project(p):
        both = win[p].reshape(pair_rows, width)
        normed = layer_norm(both.astype(F32)).astype(BF16)
        here = pl.ds(pl.multiple_of(p * pair_rows, 16), pair_rows)
        spans = width // span

        def mix(part, s):
            lo = part * width + s * span
            return dot(normed, wqkv[:, lo : lo + span])

        def unify(part, s, mixed):
            square = dot((mixed * mixed).astype(BF16), blocks[...])
            unit = mixed * lax.rsqrt(square + 1e-06)
            if part == 0:
                unit = unit * qscale[:, s * span : (s + 1) * span]
            unit = unit.astype(BF16)
            store = ks if part else qs
            store[2 * s, here] = unit[:, :lanes]
            store[2 * s + 1, here] = unit[:, lanes:]

        def keep(s, mixed):
            for k in (0, 1):
                vs[2 * s + k, here] = jnp.where(
                    valid, mixed[:, k * lanes : (k + 1) * lanes], 0.0
                ).astype(BF16)

        jobs = [(part, s) for part in (0, 1) for s in range(spans)]
        waiting = []
        for part, s in jobs:
            waiting.append((part, s, mix(part, s)))
            if len(waiting) > 1:
                unify(*waiting.pop(0))
        for s in range(spans):
            mixed = mix(2, s)
            if waiting:
                unify(*waiting.pop(0))
            keep(s, mixed)

    q_lane = iota((pair_rows, lanes), 1)
    low = q_lane < head_size
    sides = [jnp.where(low if e == 0 else ~low, 1.0, 0.0).astype(BF16) for e in (0, 1)]
    ones_all = jnp.concatenate([ones, ones], 0)

    def attend(q, k0, sink):
        here = pl.ds(pl.multiple_of(q * pair_rows, 16), pair_rows)
        q_late = (last * (q % 2)).astype(F32)
        q_region = jnp.where(
            q_lane == 2 * heads, 1 - q_late, jnp.where(q_lane == 2 * heads + 1, q_late, 0.0)
        )

        def weigh(pair):
            query = qs[pair, here]
            keys = jnp.concatenate([ks[pair, k0 : k0 + half], kx[k0 : k0 + half]], 1)
            asked = [
                jnp.concatenate(
                    [
                        query * sides[e],
                        jnp.where(q_lane // 2 == 2 * pair + e, 1.0, q_region).astype(BF16),
                    ],
                    1,
                )
                for e in (0, 1)
            ]
            soft[pair % 2] = jnp.exp2(dot_t(jnp.concatenate(asked, 0), keys)).astype(BF16)

        def gain(pair):
            values = jnp.concatenate([vs[pair, k0 : k0 + half], ones_all], 1)
            summed = dot(soft[pair % 2], values)
            up, down = summed[:pair_rows], summed[pair_rows:]
            sink(
                pair,
                jnp.where(low, up[:, :lanes], down[:, :lanes]),
                jnp.where(low, up[:, lanes:], down[:, lanes:]),
            )

        weigh(0)
        for pair in range(pairs):
            if pair + 1 < pairs:
                weigh(pair + 1)
            gain(pair)

    def attend_near(q, carry):
        def sink(pair, above, below):
            acc[q, pair, 0] = above
            acc[q, pair, 1] = below

        attend(q, 0, sink)
        return carry

    def attend_far(q):
        def sink(pair, above, below):
            ratio = (above + acc[q, pair, 0]) / (below + acc[q, pair, 1])
            att[:, pair * lanes : (pair + 1) * lanes] = ratio.astype(BF16)

        attend(q, half, sink)

    def join(p):
        projected = dot(att[...], wout[...]).astype(BF16)
        own = win[p].reshape(pair_rows, width)
        residual = (own.astype(F32) + projected.astype(F32)).astype(BF16).astype(F32)
        mlp_in = layer_norm(residual).astype(BF16)
        update = jnp.zeros_like(residual)
        hidden_size = wup.shape[1]
        piece = 512
        slope = math.sqrt(2.0 / math.pi)

        def raise_(s):
            up = dot(mlp_in, wup[:, s * piece : (s + 1) * piece])
            bent = jnp.tanh(up * (slope + 0.044715 * slope * (up * up)))
            return (up + up * bent).astype(BF16)

        pieces = hidden_size // piece
        twice = raise_(0)
        for s in range(pieces):
            later = raise_(s + 1) if s + 1 < pieces else None
            update = update + dot(twice, wdown[s * piece : (s + 1) * piece, :])
            twice = later
        joined = (residual + 0.5 * update).astype(BF16)
        flat = []
        for (token, _, held, _), put in zip(cuts, puts):
            tall = jnp.concatenate(
                [
                    jnp.concatenate(
                        [
                            joined[rr * rows + token : rr * rows + token + held, 128 * t : 128 * (t + 1)]
                            for t in range(tiles)
                        ],
                        0,
                    )
                    for rr in (0, 1)
                ],
                1,
            )
            flat.append(dot(put[...], tall).astype(BF16))
        flat = jnp.concatenate(flat, 0)
        d, other = p // 2, p % 2
        for k in (1, 0):
            rout[2 * p + k] = flat[:, 128 * k : 128 * (k + 1)].reshape(slab)
            same = 1 - last
            cc, rr = k + same * (other - k), other + same * (k - other)
            away = d + cc + rr * mine
            pl.when(away > 0)(lambda: backward(d, cc, rr).start())
            pl.when(away == 0)(lambda: settle(cc, rr).start())

    weights[0].wait()

    def mark_all():
        for n in range(3):
            pltpu.make_async_copy(marked.at[n], marked.at[n], mrecv.at[n]).wait()
        lax.fori_loop(0, 2, mark, 0)

    def gather(t, carry):
        arrive(t)
        project(t)
        pl.when(t == 1)(mark_all)
        first = jnp.where(t == 1, 0, t)
        lax.fori_loop(first, jnp.where(t == 0, 0, t + 1), attend_near, 0)
        return carry

    def scatter(t, carry):
        p = jnp.where(t == 1, 2 - last, jnp.where(t == 2, 1 + last, 3 - t))
        attend_far(p)
        join(p)
        return carry

    lax.fori_loop(0, 4, gather, 0)
    for copy in weights[1:]:
        copy.wait()
    lax.fori_loop(0, 4, scatter, 0)

    for n in range(3):
        share(n).wait_send()
    for d, cc, rr in order:
        by_owner(d, cc, rr, None, lambda: forward(d, cc, rr).wait_send())
    for d, cc, rr in order:
        by_owner(d, cc, rr, None, lambda: backward(d, cc, rr).wait_send())
    for d, cc, rr in order:
        landed = block_of(out_ref, (g + b + d + cc) % 2, cc, rr)
        pltpu.make_async_copy(landed, landed, recv2.at[4 * d + 2 * cc + rr]).wait()


def hand_over(src, dst, sem):
    gives = [pltpu.make_async_copy(src.at[i], dst.at[i], sem.at[i]) for i in range(src.shape[0])]
    for give in gives:
        give.start()
    for give in gives:
        give.wait()


def per_device(fields, surface_mask, w_qkv, w_out, logit_scale, mask_bias, w_up, w_down):
    groups, levels, nlat, nlon, width = fields.shape
    heads = logit_scale.shape[0]
    head_size = width // heads
    real = groups * levels * SH_LAT * SH_LON
    rows = -(-real // 16) * 16
    total = 8 * rows

    tiles = width // 128
    raw = fields.reshape(groups, levels, nlat, nlon, tiles, 128)
    raw = jnp.transpose(raw, (0, 2, 3, 4, 1, 5))
    raw = raw.reshape(groups, nlat, nlon // 2, 2 * tiles * levels, 128)
    slab = (groups, SH_LAT, SH_LON // 2) + raw.shape[3:]

    cut = 256 // tiles
    spans = ((256, cut * tiles), (math.prod(slab[:-1]) - 256, (rows - cut) * tiles))
    orders = [(held, flat) for flat, held in spans] + list(spans)

    vmem = pl.BlockSpec(memory_space=pltpu.VMEM)
    anywhere = pl.BlockSpec(memory_space=pl.ANY)
    joined = pl.pallas_call(
        functools.partial(kernel, real, heads),
        out_shape=pltpu.VMEM(raw.shape, BF16),
        in_specs=[anywhere] * 8,
        out_specs=anywhere,
        scratch_shapes=[
            pltpu.VMEM(raw.shape, BF16),
            pltpu.VMEM((nlat, levels, nlon), jnp.int32),
            pltpu.SMEM(logit_scale.shape, F32),
            pltpu.SMEM(mask_bias.shape, F32),
            pltpu.VMEM((nlat * levels, 128), F32),
            pltpu.VMEM((3, nlat * levels, 128), F32),
            pltpu.VMEM((8,) + slab, BF16),
            pltpu.VMEM((4, 2, rows, width), BF16),
            pltpu.VMEM(w_qkv.shape, BF16),
            pltpu.VMEM(w_out.shape, BF16),
            pltpu.VMEM(w_up.shape, BF16),
            pltpu.VMEM(w_down.shape, BF16),
            pltpu.VMEM((total // 4, width), BF16),
            pltpu.VMEM((heads // 2, total, 2 * head_size), BF16),
            pltpu.VMEM((heads // 2, total, 2 * head_size), BF16),
            pltpu.VMEM((heads // 2, total, 2 * head_size), BF16),
            pltpu.VMEM((total, 2 * head_size), BF16),
            pltpu.VMEM((4, heads // 2, 2, total // 4, 2 * head_size), F32),
            pltpu.VMEM((8,) + slab, BF16),
        ]
        + [pltpu.VMEM(shape, BF16) for shape in orders]
        + [
            pltpu.VMEM((4 * head_size, 4 * head_size), BF16),
            pltpu.VMEM((2, total // 2, total // 2), BF16),
            pltpu.SemaphoreType.DMA((5,)),
            pltpu.SemaphoreType.DMA((3,)),
            pltpu.SemaphoreType.DMA((3,)),
            pltpu.SemaphoreType.DMA((3,)),
            pltpu.SemaphoreType.DMA((8,)),
            pltpu.SemaphoreType.DMA((8,)),
            pltpu.SemaphoreType.DMA((8,)),
            pltpu.SemaphoreType.DMA((8,)),
        ],
        compiler_params=pltpu.CompilerParams(
            collective_id=0, has_side_effects=True, vmem_limit_bytes=56 * 1024 * 1024
        ),
        name="window_block",
    )(raw, jnp.transpose(surface_mask, (1, 0, 2)), logit_scale, mask_bias, w_qkv, w_out, w_up, w_down)

    joined = pl.pallas_call(
        hand_over,
        out_shape=jax.ShapeDtypeStruct(raw.shape, BF16),
        in_specs=[vmem],
        out_specs=anywhere,
        scratch_shapes=[pltpu.SemaphoreType.DMA((groups,))],
        name="hand_over",
    )(pltpu.with_memory_space_constraint(joined, pltpu.VMEM))
    joined = joined.reshape(groups, nlat, nlon, tiles, levels, 128)
    return jnp.transpose(joined, (0, 4, 1, 2, 3, 5)).reshape(fields.shape)


def solution(mesh):
    return jax.shard_map(
        per_device,
        mesh=mesh,
        in_specs=(
            P("grp", None, "lat", "lon", None),
            P(None, "lat", "lon"),
            P(),
            P(),
            P(),
            P(),
            P(),
            P(),
        ),
        out_specs=P("grp", None, "lat", "lon", None),
        check_vma=False,
    )
```

```python
import functools
import math

import jax
import jax.numpy as jnp
from jax import lax
from jax.experimental import pallas as pl
from jax.experimental.pallas import tpu as pltpu
from jax.sharding import PartitionSpec as P

SH_LAT = 3
SH_LON = 6
LOG2E = math.log2(math.e)
FAR = -30000.0
MESH = pl.DeviceIdType.MESH
BF16 = jnp.bfloat16
F32 = jnp.float32


def layer_norm(values):
    centred = values - jnp.mean(values, -1, keepdims=True)
    return centred * lax.rsqrt(jnp.mean(centred * centred, -1, keepdims=True) + 1e-05)


def iota(shape, axis):
    return lax.broadcasted_iota(jnp.int32, shape, axis)


def dot(left, right):
    return jnp.dot(left, right, preferred_element_type=F32)


def dot_t(left, right):
    return lax.dot_general(left, right, (((1,), (1,)), ((), ())), preferred_element_type=F32)


def kernel(
    real, heads,
    fields_hbm, mask_hbm, scale_hbm, bias_hbm, wqkv_hbm, wout_hbm, wup_hbm, wdown_hbm,
    out_ref,
    raw, mask_ref, scale_ref, bias_ref, tidy, marked, rin, win, wqkv, wout, wup, wdown, att, qs, ks, vs,
    kx, acc, rout, sort0, sort1, put0, put1, blocks, soft,
    wsem, ssem, msend, mrecv, send1, recv1, send2, recv2,
):
    rows, width = win.shape[2:]
    levels = mask_ref.shape[1]
    nlat = mask_ref.shape[0]
    tiles = width // 128
    side_pairs = SH_LON // 2
    slab = rin.shape[1:]
    slab_rows = slab[0] * slab[1] * slab[2] * slab[3]
    pair_rows = 2 * rows
    half = 2 * pair_rows
    total = 2 * half
    pairs = heads // 2
    head_size = width // heads
    lanes = 2 * head_size
    cut_rows = 256
    cut = cut_rows // tiles

    g, a, b = lax.axis_index("grp"), lax.axis_index("lat"), lax.axis_index("lon")
    na, nb = lax.axis_size("lat"), lax.axis_size("lon")
    mine = (g + b) % 2

    def peer(d, da, db):
        return {"grp": (g + d) % 2, "lat": (a + da + na) % na, "lon": (b + db + nb) % nb}

    barrier = pltpu.get_barrier_semaphore()
    greeted = 0
    for d in (0, 1):
        for da, db in ((0, 0), (-1, 0), (0, -1), (-1, -1), (1, 0), (0, 1), (1, 1)):
            if d or da or db:
                pl.semaphore_signal(barrier, inc=1, device_id=peer(d, da, db), device_id_type=MESH)
                greeted += 1

    last = jnp.where(a == na - 1, mine, 0)

    def slot(d, cc, rr, crossed):
        same = 1 - crossed
        return 4 * d + 2 * (rr + same * (cc - rr)) + cc + same * (rr - cc)

    def row_of(parity, rr):
        return (1 + 2 * parity + rr) % 4

    def block_of(ref, parity, cc, rr):
        r = row_of(parity, rr)
        return ref.at[:, pl.ds(SH_LAT * r, SH_LAT), pl.ds(side_pairs * (1 - cc), side_pairs)]

    def by_owner(d, cc, rr, local, remote):
        if d or cc:
            remote()
        elif rr == 0:
            if local is not None:
                local()
        else:
            pl.when(mine == 1)(remote)
            if local is not None:
                pl.when(mine == 0)(local)

    def stay(cc, rr):
        i = slot(0, cc, rr, 0)
        return pltpu.make_async_copy(block_of(fields_hbm, mine, cc, rr), rin.at[i], recv1.at[i])

    def forward(d, cc, rr):
        n = 4 * d + 2 * cc + rr
        parity = (g + b + d + cc) % 2
        i = slot(d, cc, rr, jnp.where((a - rr * parity + na) % na == na - 1, parity, 0))
        return pltpu.make_async_remote_copy(
            src_ref=block_of(raw, parity, cc, rr), dst_ref=rin.at[i],
            send_sem=send1.at[n], recv_sem=recv1.at[i],
            device_id=peer(d, -rr * parity, -cc), device_id_type=MESH,
        )

    def backward(d, cc, rr):
        n = 4 * d + 2 * cc + rr
        return pltpu.make_async_remote_copy(
            src_ref=rout.at[slot(d, cc, rr, last)], dst_ref=block_of(out_ref, mine, cc, rr),
            send_sem=send2.at[n], recv_sem=recv2.at[n],
            device_id=peer(d, rr * mine, cc), device_id_type=MESH,
        )

    def settle(cc, rr):
        n = 2 * cc + rr
        return pltpu.make_async_copy(
            rout.at[slot(0, cc, rr, last)], block_of(out_ref, mine, cc, rr), recv2.at[n]
        )

    def share(n):
        da, db = ((0, -1), (-1, 0), (-1, -1))[n]
        return pltpu.make_async_remote_copy(
            src_ref=tidy, dst_ref=marked.at[n], send_sem=msend.at[n], recv_sem=mrecv.at[n],
            device_id=peer(0, da, db), device_id_type=MESH,
        )

    load = pltpu.make_async_copy(fields_hbm, raw, wsem.at[4])
    load.start()
    small = [
        pltpu.make_async_copy(src, dst, ssem.at[i])
        for i, (src, dst) in enumerate(
            ((mask_hbm, mask_ref), (scale_hbm, scale_ref), (bias_hbm, bias_ref))
        )
    ]
    for copy in small:
        copy.start()
    stay(0, 0).start()
    pl.when(mine == 0)(lambda: stay(0, 1).start())
    weights = [
        pltpu.make_async_copy(src, dst, wsem.at[i])
        for i, (src, dst) in enumerate(
            ((wqkv_hbm, wqkv), (wout_hbm, wout), (wup_hbm, wup), (wdown_hbm, wdown))
        )
    ]

    for copy in small:
        copy.wait()
    tidy[...] = jnp.zeros_like(tidy)
    for i in range(nlat):
        tidy[levels * i : levels * (i + 1), : mask_ref.shape[2]] = mask_ref[i].astype(F32)

    load.wait()
    for copy in weights:
        copy.start()
    pl.semaphore_wait(barrier, greeted)
    for n in range(3):
        share(n).start()
    order = [(1, 0, 0), (0, 1, 0), (0, 0, 0), (0, 1, 1), (0, 0, 1)]
    order += [(1, 0, 1), (1, 1, 0), (1, 1, 1)]
    for d, cc, rr in order:
        by_owner(d, cc, rr, None, lambda: forward(d, cc, rr).start())

    def shuffle(count, held, out_rows, raw_out):
        shape = (out_rows, held * tiles) if raw_out else (held * tiles, out_rows)
        tall, flat = iota(shape, 1 if raw_out else 0), iota(shape, 0 if raw_out else 1)
        token, tile = tall % held, tall // held
        place = token // levels * (tiles * levels) + tile * levels + token % levels
        return jnp.where((place == flat) & (token < count), 1.0, 0.0).astype(BF16)

    rest = real - cut
    rest_held = rows - cut
    cuts = ((0, cut, cut, cut_rows), (cut, rest, rest_held, slab_rows - cut_rows))
    sorts, puts = (sort0, sort1), (put0, put1)
    for (_, count, held, n), pick, put in zip(cuts, sorts, puts):
        pick[...] = shuffle(count, held, n, False)
        put[...] = shuffle(count, held, n, True)

    row_in_block = iota((pair_rows, lanes), 0) % rows
    valid = row_in_block < real
    raw_bias = jnp.zeros((1, lanes), F32)
    qscale = jnp.zeros((1, width), F32)
    for h in range(heads):
        raw_bias = jnp.where(
            iota((1, lanes), 1) // 2 == h, bias_ref[h] * LOG2E, raw_bias
        )
        qscale = jnp.where(
            iota((1, width), 1) // head_size == h, scale_ref[h] * (LOG2E / head_size), qscale
        )
    bias_hi = raw_bias.astype(BF16).astype(F32)
    bias_row = jnp.where(iota(raw_bias.shape, 1) % 2 == 0, bias_hi, raw_bias - bias_hi)
    span = 2 * lanes
    blocks[...] = jnp.where(
        iota((span, span), 0) // head_size == iota((span, span), 1) // head_size,
        1.0 / head_size, 0.0,
    ).astype(BF16)
    ones = jnp.where(valid, 1.0, 0.0).astype(BF16)

    def arrive(p):
        for rr in (0, 1):
            i = 2 * p + rr
            pltpu.make_async_copy(rin.at[i], rin.at[i], recv1.at[i]).wait()
        both = jnp.concatenate([rin[2 * p + rr].reshape(slab_rows, 128) for rr in (0, 1)], 1)
        start = 0
        for (token, _, held, n), pick in zip(cuts, sorts):
            tall = dot(pick[...], both[start : start + n]).astype(BF16)
            start += n
            for rr in (0, 1):
                for t in range(tiles):
                    win[p, rr, token : token + held, 128 * t : 128 * (t + 1)] = tall[
                        t * held : (t + 1) * held, 128 * rr : 128 * (rr + 1)
                    ]

    def mark(rr, carry):
        token = iota((rows, 1), 0)
        cell = token // levels
        lane = iota((rows, lanes), 1)
        late = (rr * last).astype(F32)
        far = jnp.where(
            lane == 2 * heads, FAR * late, jnp.where(lane == 2 * heads + 1, FAR * (1 - late), 0.0)
        )
        over = (rr * mine).astype(F32)
        for cc in (0, 1):
            near = tidy[...] if cc == 0 else marked[0]
            near = near + over * (marked[1 + cc] - near)
            at_lat = (SH_LAT * row_of(mine, rr) + cell // SH_LON % SH_LAT) * levels + token % levels
            at_lon = (1 - cc) * SH_LON + cell % SH_LON
            by_lat = jnp.where(iota((rows, tidy.shape[0]), 1) == at_lat, 1.0, 0.0).astype(BF16)
            by_cell = dot(by_lat, near.astype(BF16))
            by_cell = jnp.where(iota((rows, 128), 1) == at_lon, by_cell, 0.0).astype(BF16)
            marks = dot(by_cell, jnp.ones((128, lanes), BF16))
            key = (marks * bias_row + far).astype(BF16)
            for d in (0, 1):
                at = pl.multiple_of(slot(d, cc, rr, last) * rows, 16)
                kx[pl.ds(at, rows)] = key
        return carry

    def project(p):
        both = win[p].reshape(pair_rows, width)
        normed = layer_norm(both.astype(F32)).astype(BF16)
        here = pl.ds(pl.multiple_of(p * pair_rows, 16), pair_rows)
        spans = width // span

        def mix(part, s):
            lo = part * width + s * span
            return dot(normed, wqkv[:, lo : lo + span])

        def unify(part, s, mixed):
            square = dot((mixed * mixed).astype(BF16), blocks[...])
            unit = mixed * lax.rsqrt(square + 1e-06)
            if part == 0:
                unit = unit * qscale[:, s * span : (s + 1) * span]
            unit = unit.astype(BF16)
            store = ks if part else qs
            store[2 * s, here] = unit[:, :lanes]
            store[2 * s + 1, here] = unit[:, lanes:]

        def keep(s, mixed):
            for k in (0, 1):
                vs[2 * s + k, here] = jnp.where(
                    valid, mixed[:, k * lanes : (k + 1) * lanes], 0.0
                ).astype(BF16)

        jobs = [(part, s) for part in (0, 1) for s in range(spans)]
        waiting = []
        for part, s in jobs:
            waiting.append((part, s, mix(part, s)))
            if len(waiting) > 1:
                unify(*waiting.pop(0))
        for s in range(spans):
            mixed = mix(2, s)
            if waiting:
                unify(*waiting.pop(0))
            keep(s, mixed)

    q_lane = iota((pair_rows, lanes), 1)
    low = q_lane < head_size
    sides = [jnp.where(low if e == 0 else ~low, 1.0, 0.0).astype(BF16) for e in (0, 1)]
    ones_all = jnp.concatenate([ones, ones], 0)

    def attend(q, k0, sink):
        here = pl.ds(pl.multiple_of(q * pair_rows, 16), pair_rows)
        q_late = (last * (q % 2)).astype(F32)
        q_region = jnp.where(
            q_lane == 2 * heads, 1 - q_late, jnp.where(q_lane == 2 * heads + 1, q_late, 0.0)
        )

        def weigh(pair):
            query = qs[pair, here]
            keys = jnp.concatenate([ks[pair, k0 : k0 + half], kx[k0 : k0 + half]], 1)
            asked = [
                jnp.concatenate(
                    [
                        query * sides[e],
                        jnp.where(q_lane // 2 == 2 * pair + e, 1.0, q_region).astype(BF16),
                    ],
                    1,
                )
                for e in (0, 1)
            ]
            soft[pair % 2] = jnp.exp2(dot_t(jnp.concatenate(asked, 0), keys)).astype(BF16)

        def gain(pair):
            values = jnp.concatenate([vs[pair, k0 : k0 + half], ones_all], 1)
            summed = dot(soft[pair % 2], values)
            up, down = summed[:pair_rows], summed[pair_rows:]
            sink(
                pair,
                jnp.where(low, up[:, :lanes], down[:, :lanes]),
                jnp.where(low, up[:, lanes:], down[:, lanes:]),
            )

        weigh(0)
        for pair in range(pairs):
            if pair + 1 < pairs:
                weigh(pair + 1)
            gain(pair)

    def attend_near(q, carry):
        def sink(pair, above, below):
            acc[q, pair, 0] = above
            acc[q, pair, 1] = below

        attend(q, 0, sink)
        return carry

    def attend_far(q):
        def sink(pair, above, below):
            ratio = (above + acc[q, pair, 0]) / (below + acc[q, pair, 1])
            att[:, pair * lanes : (pair + 1) * lanes] = ratio.astype(BF16)

        attend(q, half, sink)

    def join(p):
        projected = dot(att[...], wout[...]).astype(BF16)
        own = win[p].reshape(pair_rows, width)
        residual = (own.astype(F32) + projected.astype(F32)).astype(BF16).astype(F32)
        mlp_in = layer_norm(residual).astype(BF16)
        update = jnp.zeros_like(residual)
        hidden_size = wup.shape[1]
        piece = 512
        slope = math.sqrt(2.0 / math.pi)

        def raise_(s):
            up = dot(mlp_in, wup[:, s * piece : (s + 1) * piece])
            bent = jnp.tanh(up * (slope + 0.044715 * slope * (up * up)))
            return (up + up * bent).astype(BF16)

        pieces = hidden_size // piece
        twice = raise_(0)
        for s in range(pieces):
            later = raise_(s + 1) if s + 1 < pieces else None
            update = update + dot(twice, wdown[s * piece : (s + 1) * piece, :])
            twice = later
        joined = (residual + 0.5 * update).astype(BF16)
        flat = []
        for (token, _, held, _), put in zip(cuts, puts):
            tall = jnp.concatenate(
                [
                    jnp.concatenate(
                        [
                            joined[rr * rows + token : rr * rows + token + held, 128 * t : 128 * (t + 1)]
                            for t in range(tiles)
                        ],
                        0,
                    )
                    for rr in (0, 1)
                ],
                1,
            )
            flat.append(dot(put[...], tall).astype(BF16))
        flat = jnp.concatenate(flat, 0)
        d, other = p // 2, p % 2
        for k in (1, 0):
            rout[2 * p + k] = flat[:, 128 * k : 128 * (k + 1)].reshape(slab)
            same = 1 - last
            cc, rr = k + same * (other - k), other + same * (k - other)
            away = d + cc + rr * mine
            pl.when(away > 0)(lambda: backward(d, cc, rr).start())
            pl.when(away == 0)(lambda: settle(cc, rr).start())

    weights[0].wait()

    def mark_all():
        for n in range(3):
            pltpu.make_async_copy(marked.at[n], marked.at[n], mrecv.at[n]).wait()
        lax.fori_loop(0, 2, mark, 0)

    def gather(t, carry):
        arrive(t)
        project(t)
        pl.when(t == 1)(mark_all)
        first = jnp.where(t == 1, 0, t)
        lax.fori_loop(first, jnp.where(t == 0, 0, t + 1), attend_near, 0)
        return carry

    def scatter(t, carry):
        p = jnp.where(t == 1, 2 - last, jnp.where(t == 2, 1 + last, 3 - t))
        attend_far(p)
        join(p)
        return carry

    lax.fori_loop(0, 4, gather, 0)
    for copy in weights[1:]:
        copy.wait()
    lax.fori_loop(0, 4, scatter, 0)

    for n in range(3):
        share(n).wait_send()
    for d, cc, rr in order:
        by_owner(d, cc, rr, None, lambda: forward(d, cc, rr).wait_send())
    for d, cc, rr in order:
        by_owner(d, cc, rr, None, lambda: backward(d, cc, rr).wait_send())
    for d, cc, rr in order:
        landed = block_of(out_ref, (g + b + d + cc) % 2, cc, rr)
        pltpu.make_async_copy(landed, landed, recv2.at[4 * d + 2 * cc + rr]).wait()


def hand_over(src, dst, sem):
    gives = [pltpu.make_async_copy(src.at[i], dst.at[i], sem.at[i]) for i in range(src.shape[0])]
    for give in gives:
        give.start()
    for give in gives:
        give.wait()


def per_device(fields, surface_mask, w_qkv, w_out, logit_scale, mask_bias, w_up, w_down):
    groups, levels, nlat, nlon, width = fields.shape
    heads = logit_scale.shape[0]
    head_size = width // heads
    real = groups * levels * SH_LAT * SH_LON
    rows = -(-real // 16) * 16
    total = 8 * rows

    tiles = width // 128
    raw = fields.reshape(groups, levels, nlat, nlon, tiles, 128)
    raw = jnp.transpose(raw, (0, 2, 3, 4, 1, 5))
    raw = raw.reshape(groups, nlat, nlon // 2, 2 * tiles * levels, 128)
    slab = (groups, SH_LAT, SH_LON // 2) + raw.shape[3:]

    cut = 256 // tiles
    spans = ((256, cut * tiles), (math.prod(slab[:-1]) - 256, (rows - cut) * tiles))
    orders = [(held, flat) for flat, held in spans] + list(spans)

    vmem = pl.BlockSpec(memory_space=pltpu.VMEM)
    anywhere = pl.BlockSpec(memory_space=pl.ANY)
    joined = pl.pallas_call(
        functools.partial(kernel, real, heads),
        out_shape=pltpu.VMEM(raw.shape, BF16),
        in_specs=[anywhere] * 8,
        out_specs=anywhere,
        scratch_shapes=[
            pltpu.VMEM(raw.shape, BF16),
            pltpu.VMEM((nlat, levels, nlon), jnp.int32),
            pltpu.SMEM(logit_scale.shape, F32),
            pltpu.SMEM(mask_bias.shape, F32),
            pltpu.VMEM((nlat * levels, 128), F32),
            pltpu.VMEM((3, nlat * levels, 128), F32),
            pltpu.VMEM((8,) + slab, BF16),
            pltpu.VMEM((4, 2, rows, width), BF16),
            pltpu.VMEM(w_qkv.shape, BF16),
            pltpu.VMEM(w_out.shape, BF16),
            pltpu.VMEM(w_up.shape, BF16),
            pltpu.VMEM(w_down.shape, BF16),
            pltpu.VMEM((total // 4, width), BF16),
            pltpu.VMEM((heads // 2, total, 2 * head_size), BF16),
            pltpu.VMEM((heads // 2, total, 2 * head_size), BF16),
            pltpu.VMEM((heads // 2, total, 2 * head_size), BF16),
            pltpu.VMEM((total, 2 * head_size), BF16),
            pltpu.VMEM((4, heads // 2, 2, total // 4, 2 * head_size), F32),
            pltpu.VMEM((8,) + slab, BF16),
        ]
        + [pltpu.VMEM(shape, BF16) for shape in orders]
        + [
            pltpu.VMEM((4 * head_size, 4 * head_size), BF16),
            pltpu.VMEM((2, total // 2, total // 2), BF16),
            pltpu.SemaphoreType.DMA((5,)),
            pltpu.SemaphoreType.DMA((3,)),
            pltpu.SemaphoreType.DMA((3,)),
            pltpu.SemaphoreType.DMA((3,)),
            pltpu.SemaphoreType.DMA((8,)),
            pltpu.SemaphoreType.DMA((8,)),
            pltpu.SemaphoreType.DMA((8,)),
            pltpu.SemaphoreType.DMA((8,)),
        ],
        compiler_params=pltpu.CompilerParams(
            collective_id=0, has_side_effects=True, vmem_limit_bytes=56 * 1024 * 1024
        ),
        name="window_block",
    )(raw, jnp.transpose(surface_mask, (1, 0, 2)), logit_scale, mask_bias, w_qkv, w_out, w_up, w_down)

    joined = pl.pallas_call(
        hand_over,
        out_shape=jax.ShapeDtypeStruct(raw.shape, BF16),
        in_specs=[vmem],
        out_specs=anywhere,
        scratch_shapes=[pltpu.SemaphoreType.DMA((groups,))],
        name="hand_over",
    )(pltpu.with_memory_space_constraint(joined, pltpu.VMEM))
    joined = joined.reshape(groups, nlat, nlon, tiles, levels, 128)
    return jnp.transpose(joined, (0, 4, 1, 2, 3, 5)).reshape(fields.shape)


def solution(mesh):
    return jax.shard_map(
        per_device,
        mesh=mesh,
        in_specs=(
            P("grp", None, "lat", "lon", None),
            P(None, "lat", "lon"),
            P(),
            P(),
            P(),
            P(),
            P(),
            P(),
        ),
        out_specs=P("grp", None, "lat", "lon", None),
        check_vma=False,
    )
```
